256 devices in a mesh: tm: 32 (over z, y_lo, core), mom: 8 (over x, y_hi).
Axes of the slice: x: 4, y: 4 (y_hi: 2, y_lo: 2; y = y_hi * 2 + y_lo), z: 8, core: 2. Of those that a mesh axis runs over, the one named last changes fastest.
Arguments:
- sink_solutions: bfloat16 [32, 2, 512, 512], P('tm'), may hold values from -0.44921875 to 0.44921875
- noise_sources: bfloat16 [32, 2, 512, 512], P('tm'), may hold values from -0.44921875 to 0.44921875
- elementals: bfloat16 [8, 32, 2, 128, 128], P('mom', 'tm'), may hold values from -0.375 to 0.375
- pairs: int32 [8, 2], P('mom'), may hold values from 0 to 7
Outputs:
- blocks: bfloat16 [32, 4, 8, 2, 512, 512], P('tm', None, 'mom')
The draws below stay inside these ranges and needn't reach their ends.
Inputs may be any that keep to these rules, and one draw needn't show every extreme that they name: `pairs`: entries are operator indices.
All inputs are finite; a program needn't handle non-finite values.
Results may differ from the reference program's by a relative error of at most 0.007.
Values may be sent and summed in bfloat16 or wider, within the bound.
No kernel may reach another device: no remote copies, remote signals or barrier semaphores. Data moves between devices by JAX's collectives and lax.ppermute only.
A program may use at most 64 MiB of HBM per device.

```python
import jax
import jax.numpy as jnp
from jax import lax

NEV = 128
EIGEN_SPIN_SIZE = 512
DILUTION_INDICES = 512
NSEP = 4
TIME_SLICES = 32
NOP = 8
NPAIR = 8


def with_ends(entries, stream_key, low, high):
    spot = [jax.random.randint(jax.random.fold_in(stream_key, axis), (), 0, length) for axis, length in enumerate(entries.shape)]
    widest = entries.shape.index(max(entries.shape))
    neighbour = spot[:widest] + [(spot[widest] + 1) % entries.shape[widest]] + spot[widest + 1:]
    return entries.at[tuple(spot)].set(low).at[tuple(neighbour)].set(high)


def levels(stream_key, dims, split, smallest, high):
    level, own = 1.0, jax.random.fold_in(stream_key, 6)
    for dim, parts in split:
        heights = jnp.exp(jax.random.uniform(jax.random.fold_in(own, dim), (parts,), jnp.float32, smallest / len(split), high / len(split)))
        level = level * jnp.repeat(heights, dims[dim] // parts).reshape([-1 if axis == dim else 1 for axis in range(len(dims))])
    return level


def normal_values(key, extent, spread, reach, split=(), kind=jnp.bfloat16):
    entries = spread * jax.random.normal(key, extent, jnp.float32)
    if split:
        entries = entries * levels(key, extent, split, -0.22, 0.18)
    return jnp.clip(entries, -reach, reach).astype(kind)


def setup_inputs(seed: int = 0) -> dict:
    key_list = jax.random.split(jax.random.key(seed), 5)
    return {
        "sink_solutions": normal_values(key_list[0], (TIME_SLICES, 2, DILUTION_INDICES, EIGEN_SPIN_SIZE), 0.075, 0.44921875, ((0, 32),)),
        "noise_sources": normal_values(key_list[1], (TIME_SLICES, 2, DILUTION_INDICES, EIGEN_SPIN_SIZE), 0.075, 0.44921875, ((0, 32),)),
        "elementals": normal_values(key_list[2], (NOP, TIME_SLICES, 2, NEV, NEV), (2 * NEV) ** -0.5, 0.375, ((0, 8), (1, 32))),
        "pairs": with_ends(jax.random.randint(key_list[3], (NPAIR, 2), 0, NOP), jax.random.fold_in(key_list[3], 1), 0, NOP - 1).astype(jnp.int32),
    }


def transpose_product(left_mat, right_mat):
    return lax.dot_general(left_mat, right_mat, (((1,), (1,)), ((), ())), preferred_element_type=jnp.float32)


def complex_product(left_mat, right_mat):
    real_part = jnp.dot(left_mat[0], right_mat[0], preferred_element_type=jnp.float32) - jnp.dot(left_mat[1], right_mat[1], preferred_element_type=jnp.float32)
    imag_part = jnp.dot(left_mat[0], right_mat[1], preferred_element_type=jnp.float32) + jnp.dot(left_mat[1], right_mat[0], preferred_element_type=jnp.float32)
    return jnp.stack([real_part, imag_part])


def meson_function(sink_piece, noise_part, elemental):
    dilution_rows = sink_piece.shape[1]
    total_width = sink_piece.shape[2]
    eigenvector_count = elemental.shape[1]
    spinor_rows = sink_piece.reshape(2, dilution_rows * (total_width // eigenvector_count), eigenvector_count)
    applied_real = transpose_product(spinor_rows[0], elemental[0]) - transpose_product(spinor_rows[1], elemental[1])
    applied_imaginary = transpose_product(spinor_rows[0], elemental[1]) + transpose_product(spinor_rows[1], elemental[0])
    applied_result = jnp.stack([applied_real, applied_imaginary]).reshape(2, dilution_rows, total_width).astype(jnp.bfloat16)
    meson_re = transpose_product(noise_part[0], applied_result[0]) + transpose_product(noise_part[1], applied_result[1])
    meson_im = transpose_product(noise_part[0], applied_result[1]) - transpose_product(noise_part[1], applied_result[0])
    return jnp.stack([meson_re, meson_im]).astype(jnp.bfloat16)


def reference(sink_solutions, noise_sources, elementals, pairs):
    slice_times = jnp.arange(TIME_SLICES, dtype=jnp.int32)

    def mesons_at(slice_time):
        return lax.map(lambda operator: meson_function(sink_solutions[slice_time], noise_sources[slice_time], elementals[operator, slice_time]), jnp.arange(NOP, dtype=jnp.int32))

    mesons = lax.map(mesons_at, slice_times)

    def blocks_at(source_time):
        source_side = mesons[source_time][pairs[:, 1]]
        results = []
        for separation in range(1, NSEP + 1):
            later_time = ((source_time + separation) % TIME_SLICES).astype(jnp.int32)
            sink_side = mesons[later_time][pairs[:, 0]]
            results.append(jax.vmap(complex_product)(sink_side, source_side).astype(jnp.bfloat16))
        return jnp.stack(results)

    return lax.map(blocks_at, slice_times)
```

```python
import functools

import jax
import jax.numpy as jnp
from jax import lax
from jax.experimental import pallas as pl
from jax.experimental.pallas import tpu as pltpu
from jax.sharding import PartitionSpec as P

NSEP = 4
VMEM_LIMIT = 24 * 1024 * 1024
F32 = jnp.float32
BF16 = jnp.bfloat16


def transpose_product(left_mat, right_mat):
    return lax.dot_general(
        left_mat, right_mat, (((1,), (1,)), ((), ())), preferred_element_type=F32
    )


def params():
    return pltpu.CompilerParams(vmem_limit_bytes=VMEM_LIMIT)


def cost(flops, moved):
    return pl.CostEstimate(flops=flops, bytes_accessed=moved, transcendentals=0)


def outgoing_kernel(copies, x_ref, phi_ref, rho_ref, elem_ref, piece_ref, spread_ref):
    del x_ref
    piece_ref[0:2] = phi_ref[0]
    piece_ref[2:4] = rho_ref[0]
    for copy in range(copies):
        spread_ref[copy] = elem_ref[0, 0]


def outgoing(sink, noise, elementals, spin, copies):
    rows, nev = sink.shape[2], elementals.shape[3]
    column = pl.BlockSpec((1, 2, rows, nev), lambda i, s: (0, 0, 0, s[0]))
    return pl.pallas_call(
        functools.partial(outgoing_kernel, copies),
        grid_spec=pltpu.PrefetchScalarGridSpec(
            num_scalar_prefetch=1,
            grid=(1,),
            in_specs=[
                column,
                column,
                pl.BlockSpec((1, 1, 2, nev, nev), lambda i, s: (0, 0, 0, 0, 0)),
            ],
            out_specs=[
                pl.BlockSpec((4, rows, nev), lambda i, s: (0, 0, 0)),
                pl.BlockSpec((copies, 2, nev, nev), lambda i, s: (0, 0, 0, 0)),
            ],
        ),
        out_shape=[
            jax.ShapeDtypeStruct((4, rows, nev), BF16),
            jax.ShapeDtypeStruct((copies, 2, nev, nev), BF16),
        ],
        compiler_params=params(),
        cost_estimate=cost(1_000_000, 2_000_000),
        name="outgoing",
    )(spin, sink, noise, elementals)


def apply_weights(elem_ref):
    re, im = elem_ref[0], elem_ref[1]
    return jnp.concatenate(
        [jnp.concatenate([re, -im], axis=1), jnp.concatenate([im, re], axis=1)], axis=0
    )


def meson_from(columns, weights, out_ref):
    real = imag = None
    nev = weights.shape[0] // 2
    for phi_re, phi_im, rho_re, rho_im in columns:
        applied = transpose_product(
            jnp.concatenate([phi_re, phi_im], axis=1), weights
        ).astype(BF16)
        turned = jnp.concatenate([applied[:, nev:], -applied[:, :nev]], axis=1)
        rho = jnp.concatenate([rho_re, rho_im], axis=1)
        term_re = transpose_product(rho, applied)
        term_im = transpose_product(rho, turned)
        real = term_re if real is None else real + term_re
        imag = term_im if imag is None else imag + term_im
    out_ref[0] = real.astype(BF16)
    out_ref[1] = imag.astype(BF16)


def own_meson_kernel(which_ref, phi_ref, rho_ref, elem_ref, out_ref):
    del which_ref
    nev = elem_ref.shape[2]
    columns = []
    for spin in range(phi_ref.shape[3] // nev):
        cols = slice(spin * nev, (spin + 1) * nev)
        columns.append(
            (phi_ref[0, 0, :, cols], phi_ref[0, 1, :, cols], rho_ref[0, 0, :, cols], rho_ref[0, 1, :, cols])
        )
    meson_from(columns, apply_weights(elem_ref.at[0]), out_ref)


def own_meson(sink, noise, elementals, which):
    rows, width, nev = sink.shape[2], sink.shape[3], elementals.shape[2]
    whole = pl.BlockSpec((1, 2, rows, width), lambda i, w: (0, 0, 0, 0))
    return pl.pallas_call(
        own_meson_kernel,
        grid_spec=pltpu.PrefetchScalarGridSpec(
            num_scalar_prefetch=1,
            grid=(1,),
            in_specs=[
                whole,
                whole,
                pl.BlockSpec((1, 2, nev, nev), lambda i, w: (w[0], 0, 0, 0)),
            ],
            out_specs=pl.BlockSpec((2, rows, rows), lambda i, w: (0, 0, 0)),
        ),
        out_shape=jax.ShapeDtypeStruct((2, rows, rows), BF16),
        compiler_params=params(),
        cost_estimate=cost(1_340_000_000, 3_200_000),
        name="own_meson",
    )(which, sink, noise, elementals)


def piece_meson_kernel(*refs):
    *pieces, elem_ref, out_ref = refs
    columns = [tuple(piece[i] for i in range(4)) for piece in pieces]
    meson_from(columns, apply_weights(elem_ref), out_ref)


def piece_meson(pieces, elemental):
    rows = pieces[0].shape[1]
    return pl.pallas_call(
        piece_meson_kernel,
        in_specs=[pl.BlockSpec(memory_space=pltpu.VMEM)] * (len(pieces) + 1),
        out_specs=pl.BlockSpec(memory_space=pltpu.VMEM),
        out_shape=jax.ShapeDtypeStruct((2, rows, rows), BF16),
        compiler_params=params(),
        cost_estimate=cost(1_340_000_000, 3_200_000),
        name="piece_meson",
    )(*pieces, elemental)


def multiply(left, right_ref, out_ref):
    left = jnp.concatenate([left[0], left[1]], axis=1)
    re, im = right_ref[0], right_ref[1]
    out_ref[0, 0, 0, 0] = jnp.dot(
        left, jnp.concatenate([re, -im], axis=0), preferred_element_type=F32
    ).astype(BF16)
    out_ref[0, 0, 0, 1] = jnp.dot(
        left, jnp.concatenate([im, re], axis=0), preferred_element_type=F32
    ).astype(BF16)


def product_kernel(where_ref, left_ref, right_ref, *rest):
    del where_ref
    multiply(left_ref, right_ref, rest[-1])


def choice_kernel(where_ref, first_ref, second_ref, right_ref, *rest):
    left = jnp.where(where_ref[1] == 0, first_ref[...], second_ref[...])
    multiply(left, right_ref, rest[-1])


def product(where, lefts, right, held):
    rows = right.shape[1]
    whole = pl.BlockSpec((2, rows, rows), lambda i, w: (0, 0, 0))
    operands = [where, *lefts, right] + ([] if held is None else [held])
    return pl.pallas_call(
        product_kernel if len(lefts) == 1 else choice_kernel,
        grid_spec=pltpu.PrefetchScalarGridSpec(
            num_scalar_prefetch=1,
            grid=(1,),
            in_specs=[whole] * (len(lefts) + 1)
            + ([] if held is None else [pl.BlockSpec(memory_space=pl.ANY)]),
            out_specs=pl.BlockSpec(
                (1, 1, 1, 2, rows, rows), lambda i, w: (0, w[0], 0, 0, 0, 0)
            ),
        ),
        out_shape=jax.ShapeDtypeStruct((1, NSEP, 1, 2, rows, rows), BF16),
        input_output_aliases={} if held is None else {len(operands) - 1: 0},
        compiler_params=params(),
        cost_estimate=cost(1_080_000_000, 3_200_000),
        name="product",
    )(*operands)


def local(sink, noise, elementals, pairs):
    times, moms = lax.axis_size("tm"), lax.axis_size("mom")
    core = lax.axis_index("tm") % 2
    column = lax.axis_index("mom") // 2
    spins = sink.shape[3] // elementals.shape[3]

    def earlier(block, distance, keep=lambda t: True):
        route = [(t, (t - distance) % times) for t in range(times) if keep(t)]
        return lax.ppermute(block, "tm", route)

    def partner(block, keep=lambda t: True):
        return lax.ppermute(block, "tm", [(t, t ^ 1) for t in range(times) if keep(t)])

    def along_x(block, distance):
        count = moms // 2
        route = [(m, (m // 2 + distance) % count * 2 + m % 2) for m in range(moms)]
        return lax.ppermute(block, "mom", route)

    def scalars(*values):
        return jnp.stack([jnp.asarray(value, jnp.int32) for value in values])

    pairs = jnp.clip(pairs, 0, moms - 1)
    piece, spread = outgoing(sink, noise, elementals, scalars(column % spins), moms)
    gathered = lax.all_to_all(spread, "mom", 0, 0, tiled=True)
    piece = earlier(piece, 2)
    pieces = [piece] + [along_x(piece, distance) for distance in (1, 3, 2)]

    sink_elemental = lax.dynamic_index_in_dim(gathered, pairs[0, 0], 0, keepdims=False)
    later_elemental = earlier(sink_elemental, 2)
    sink_meson = own_meson(sink, noise, gathered, pairs[0, 0:1])
    four_later = earlier(sink_meson, 4)
    one_later = partner(sink_meson, lambda t: t % 2 == 1)
    source_meson = own_meson(sink, noise, gathered, pairs[0, 1:2])

    two_later = piece_meson(pieces, later_elemental)
    beside_two = partner(two_later)
    three_later = partner(four_later, lambda t: t % 2 == 0)

    blocks = product(scalars(1), [two_later], source_meson, None)
    blocks = product(scalars(2 - 2 * core), [beside_two], source_meson, blocks)
    blocks = product(scalars(3), [four_later], source_meson, blocks)
    return product(scalars(2 * core, core), [one_later, three_later], source_meson, blocks)


def solution(mesh):
    return jax.shard_map(
        local,
        mesh=mesh,
        in_specs=(
            P("tm", None, None, None),
            P("tm", None, None, None),
            P("mom", "tm", None, None, None),
            P("mom", None),
        ),
        out_specs=P("tm", None, "mom", None, None, None),
        check_vma=False,
    )
```

```python
import functools

import jax
import jax.numpy as jnp
from jax import lax
from jax.experimental import pallas as pl
from jax.experimental.pallas import tpu as pltpu
from jax.sharding import PartitionSpec as P


NSEP = 4
VMEM_LIMIT = 24 * 1024 * 1024
F32 = jnp.float32
BF16 = jnp.bfloat16
VMEM, SMEM, HBM = pltpu.VMEM, pltpu.SMEM, pltpu.HBM
DMA = pltpu.SemaphoreType.DMA


def transpose_product(left_mat, right_mat):
    return lax.dot_general(
        left_mat, right_mat, (((1,), (1,)), ((), ())), preferred_element_type=F32
    )


def in_space(space, count=1):
    return [pl.BlockSpec(memory_space=space)] * count


def fixed(array, space):
    return pltpu.with_memory_space_constraint(array, space)


def kernel_call(body, flops, in_specs, out_shape, scratch=(), **options):
    many = isinstance(out_shape, list)
    spaces = [in_space(shape.memory_space)[0] for shape in (out_shape if many else [out_shape])]
    return pl.pallas_call(
        body,
        in_specs=in_specs,
        out_specs=spaces if many else spaces[0],
        out_shape=out_shape,
        scratch_shapes=scratch,
        compiler_params=pltpu.CompilerParams(vmem_limit_bytes=VMEM_LIMIT),
        cost_estimate=pl.CostEstimate(flops=flops, bytes_accessed=3_000_000, transcendentals=0),
        **options,
    )


def outgoing_kernel(mom_ref, time_ref, phi_hbm, rho_hbm, piece_ref, sems):
    del time_ref
    nev = piece_ref.shape[2]
    cols = pl.ds(pl.multiple_of(mom_ref[0] // 2 * nev, nev), nev)
    copies = [
        pltpu.make_async_copy(
            source.at[0, part, :, cols], piece_ref.at[2 * which + part], sems.at[2 * which + part]
        )
        for which, source in enumerate((phi_hbm, rho_hbm))
        for part in range(2)
    ]
    for copy in copies:
        copy.start()
    for copy in copies:
        copy.wait()


def outgoing(mom, time, sink, noise, nev):
    rows = sink.shape[2]
    return kernel_call(
        outgoing_kernel,
        1_000_000,
        in_space(SMEM, 2) + in_space(HBM, 2),
        VMEM((4, rows, nev), BF16),
        [DMA((4,))],
    )(mom, time, fixed(sink, HBM), fixed(noise, HBM))


def stage_kernel(phi_hbm, rho_hbm, phi, rho, sems):
    spins, nev = phi.shape[0], phi.shape[2] // 2
    copies = []
    for source, held in ((phi_hbm, phi), (rho_hbm, rho)):
        for spin in range(spins):
            for part in range(2):
                copies.append(
                    pltpu.make_async_copy(
                        source.at[0, part, :, pl.ds(spin * nev, nev)],
                        held.at[spin, :, pl.ds(part * nev, nev)],
                        sems.at[len(copies)],
                    )
                )
                copies[-1].start()
    for copy in copies:
        copy.wait()


def stage(sink, noise, nev):
    rows, width = sink.shape[2:]
    spins = width // nev
    return kernel_call(
        stage_kernel,
        1_000_000,
        in_space(HBM, 2),
        [VMEM((spins, rows, 2 * nev), BF16)] * 2,
        [DMA((4 * spins,))],
    )(fixed(sink, HBM), fixed(noise, HBM))


def fill_weights(elem, weights):
    nev = elem.shape[1]
    re, im = elem[0], elem[1]
    weights[:nev, :nev], weights[:nev, nev:] = re, -im
    weights[nev:, :nev], weights[nev:, nev:] = im, re


def apply_elemental(phi, weights, right, at):
    nev = phi.shape[1] // 2
    applied = transpose_product(weights, phi).astype(BF16)
    right[0, at : at + 2 * nev] = applied
    right[1, at : at + nev] = applied[nev:]
    right[1, at + nev : at + 2 * nev] = -applied[:nev]


def plain_product(left, right):
    return jnp.dot(left, right, preferred_element_type=F32)


def own_meson_kernel(which, columns, pairs_ref, mom_ref, phi, rho, own_hbm, *refs):
    *others, out_ref, chosen, weights, right, sem = refs
    spins, nev = phi.shape[0], phi.shape[2] // 2
    own_copy = pltpu.make_async_copy(own_hbm.at[0, 0], chosen, sem)
    own_copy.start()
    wanted, mom = pairs_ref[0, which], mom_ref[0]
    distance = lax.rem(mom // 2 - wanted // 2 + columns, columns)
    slot = distance + columns * lax.rem(wanted + mom, 2)
    own_copy.wait()
    for index, other in enumerate(others):
        @pl.when(slot == index + 1)
        def _():
            chosen[...] = other[...]

    fill_weights(chosen, weights)
    for spin in range(spins):
        apply_elemental(phi[spin], weights[...], right, spin * 2 * nev)
    left = jnp.concatenate([rho[spin] for spin in range(spins)], axis=1)
    for part in range(2):
        out_ref[part] = plain_product(left, right[part]).astype(BF16)


def own_meson(which, pairs, mom, phi, rho, elementals, others):
    spins, rows, nev = phi.shape[0], phi.shape[1], phi.shape[2] // 2
    return kernel_call(
        functools.partial(own_meson_kernel, which, (len(others) + 1) // 2),
        1_340_000_000,
        in_space(SMEM, 2) + in_space(VMEM, 2) + in_space(HBM) + in_space(VMEM, len(others)),
        [VMEM((2, rows, rows), BF16), VMEM((2, nev, nev), BF16)],
        [VMEM((2 * nev, 2 * nev), BF16), VMEM((2, spins * 2 * nev, rows), BF16), DMA],
    )(fixed(pairs, HBM), mom, phi, rho, fixed(elementals, HBM), *others)


def pieces_kernel(count, *refs):
    pieces, elem_ref = refs[:count], refs[count]
    before = refs[count + 1 : -3]
    out_ref, weights, right = refs[-3:]
    nev = elem_ref.shape[1]
    fill_weights(elem_ref, weights)
    for index, piece in enumerate(pieces):
        phi = jnp.concatenate([piece[0], piece[1]], axis=1)
        apply_elemental(phi, weights[...], right, index * 2 * nev)
    left = jnp.concatenate([piece[part] for piece in pieces for part in (2, 3)], axis=1)
    for part in range(2):
        term = plain_product(left, right[part])
        out_ref[part] = (term + before[0][part] if before else term).astype(out_ref.dtype)


def meson_of_pieces(pieces, elemental, before, kind):
    rows, nev = pieces[0].shape[1:]
    operands = [*pieces, elemental, *before]
    return kernel_call(
        functools.partial(pieces_kernel, len(pieces)),
        340_000_000 * len(pieces),
        in_space(VMEM, len(operands)),
        VMEM((2, rows, rows), kind),
        [VMEM((2 * nev, 2 * nev), BF16), VMEM((2, 2 * nev * len(pieces), rows), BF16)],
    )(*operands)


def product_kernel(place, choices, time_ref, *refs):
    lefts, right = refs[:choices], refs[choices]
    out_hbm, held, sems = refs[-3:]
    core = lax.rem(time_ref[0], 2)
    rows = right.shape[1]
    half = rows // 2
    copies = []
    for step in range(2):
        lines = pl.ds(step * half, half)
        left = [ref[:, lines] for ref in lefts]
        left = left[0] if choices == 1 else jnp.where(core == 0, *left)
        for part in range(2):
            if part == 0:
                term = plain_product(left[0], right[0]) - plain_product(left[1], right[1])
            else:
                term = plain_product(left[0], right[1]) + plain_product(left[1], right[0])
            held[part, lines] = term.astype(BF16)
            copies.append(
                pltpu.make_async_copy(
                    held.at[part, lines], out_hbm.at[0, place(core), 0, part, lines], sems.at[len(copies)]
                )
            )
            copies[-1].start()
    for copy in copies:
        copy.wait()


def product(place, time, lefts, right, blocks):
    rows = right.shape[2]
    operands = [time, *lefts, right] + ([] if blocks is None else [blocks])
    return kernel_call(
        functools.partial(product_kernel, place, len(lefts)),
        1_080_000_000,
        in_space(SMEM)
        + in_space(VMEM, len(lefts) + 1)
        + ([] if blocks is None else in_space(pl.ANY)),
        HBM((1, NSEP, 1, 2, rows, rows), BF16),
        [VMEM((2, rows, rows), BF16), DMA((4,))],
        input_output_aliases={} if blocks is None else {len(operands) - 1: 0},
    )(*operands)


def local(sink, noise, elementals, pairs):
    times, moms = lax.axis_size("tm"), lax.axis_size("mom")
    nev = elementals.shape[3]
    columns = moms // 2
    mom, time = lax.axis_index("mom").reshape(1), lax.axis_index("tm").reshape(1)

    def earlier(block, distance):
        return lax.ppermute(block, "tm", [(t, (t - distance) % times) for t in range(times)])

    def partner(block, keep=lambda t: True):
        return lax.ppermute(block, "tm", [(t, t ^ 1) for t in range(times) if keep(t)])

    def along_x(block, distance):
        route = [(m, (m // 2 + distance) % columns * 2 + m % 2) for m in range(moms)]
        return lax.ppermute(block, "mom", route)

    own = elementals[0, 0]
    across = lax.ppermute(own, "mom", [(m, m ^ 1) for m in range(moms)])
    piece = outgoing(mom, time, sink, noise, nev)
    piece = earlier(piece, 4)
    near, far = {}, {0: across}
    for distance in (1, 3, 2):
        near[distance] = along_x(own, distance)
    for distance in (1, 3, 2):
        far[distance] = along_x(across, distance)
    others = [near[d] for d in range(1, columns)] + [far[d] for d in range(columns)]

    phi, rho = stage(sink, noise, nev)

    def meson(which):
        return own_meson(which, pairs, mom, phi, rho, elementals, others)

    sink_meson, sink_elemental = meson(0)
    later_elemental = earlier(sink_elemental, 4)
    two_later = earlier(sink_meson, 2)
    pieces = {0: piece}
    for distance in (1, 3, 2):
        pieces[distance] = along_x(piece, distance)
    beside = partner(sink_meson, lambda t: t % 2 == 1)
    source_meson, _ = meson(1)

    partial_sum = meson_of_pieces([pieces[d] for d in (0, 1, 3)], later_elemental, [], F32)
    four_later = meson_of_pieces([pieces[2]], later_elemental, [partial_sum], BF16)
    beside_four = partner(four_later, lambda t: t % 2 == 0)
    beside_two = partner(two_later)

    blocks = product(lambda c: 1, time, [two_later], source_meson, None)
    blocks = product(lambda c: 3, time, [four_later], source_meson, blocks)
    blocks = product(lambda c: 2 - 2 * c, time, [beside_two], source_meson, blocks)
    return product(lambda c: 2 * c, time, [beside, beside_four], source_meson, blocks)


def solution(mesh):
    return jax.shard_map(
        local,
        mesh=mesh,
        in_specs=(
            P("tm", None, None, None),
            P("tm", None, None, None),
            P("mom", "tm", None, None, None),
            P("mom", None),
        ),
        out_specs=P("tm", None, "mom", None, None, None),
        check_vma=False,
    )
```

```python
import functools

import jax
import jax.numpy as jnp
from jax import lax
from jax.experimental import pallas as pl
from jax.experimental.pallas import tpu as pltpu
from jax.sharding import PartitionSpec as P


NSEP = 4
VMEM_LIMIT = 24 * 1024 * 1024
F32 = jnp.float32
BF16 = jnp.bfloat16
VMEM, SMEM, HBM = pltpu.VMEM, pltpu.SMEM, pltpu.HBM
DMA = pltpu.SemaphoreType.DMA


def transpose_product(left_mat, right_mat):
    return lax.dot_general(
        left_mat, right_mat, (((1,), (1,)), ((), ())), preferred_element_type=F32
    )


def in_space(space, count=1):
    return [pl.BlockSpec(memory_space=space)] * count


def fixed(array, space):
    return pltpu.with_memory_space_constraint(array, space)


def kernel_call(body, flops, in_specs, out_shape, scratch=(), **options):
    many = isinstance(out_shape, list)
    spaces = [in_space(shape.memory_space)[0] for shape in (out_shape if many else [out_shape])]
    return pl.pallas_call(
        body,
        in_specs=in_specs,
        out_specs=spaces if many else spaces[0],
        out_shape=out_shape,
        scratch_shapes=scratch,
        compiler_params=pltpu.CompilerParams(vmem_limit_bytes=VMEM_LIMIT),
        cost_estimate=pl.CostEstimate(flops=flops, bytes_accessed=3_000_000, transcendentals=0),
        **options,
    )


def outgoing_kernel(phi_hbm, rho_hbm, phi_out, rho_out, sems):
    nev = phi_out.shape[2]
    cols = pl.ds(pl.multiple_of(lax.axis_index("mom") // 2 * nev, nev), nev)
    copies = []
    for source, held in ((phi_hbm, phi_out), (rho_hbm, rho_out)):
        for part in range(2):
            copies.append(
                pltpu.make_async_copy(source.at[0, part, :, cols], held.at[part], sems.at[len(copies)])
            )
            copies[-1].start()
    for copy in copies:
        copy.wait()


def outgoing(sink, noise, nev):
    rows = sink.shape[2]
    return kernel_call(
        outgoing_kernel, 1_000_000, in_space(HBM, 2), [VMEM((2, rows, nev), BF16)] * 2, [DMA((4,))]
    )(fixed(sink, HBM), fixed(noise, HBM))


def by_spin(source, held, sems):
    spins, nev = held.shape[0], held.shape[2] // 2
    return [
        pltpu.make_async_copy(
            source.at[0, part, :, pl.ds(spin * nev, nev)],
            held.at[spin, :, pl.ds(part * nev, nev)],
            sems.at[2 * spin + part],
        )
        for spin in range(spins)
        for part in range(2)
    ]


def stage_kernel(phi_hbm, rho_hbm, elem_hbm, phi, rho, elem, sems):
    count = sems.shape[0] // 2
    copies = by_spin(phi_hbm, phi, sems) + by_spin(rho_hbm, rho, sems.at[pl.ds(count, count)])
    copies.append(pltpu.make_async_copy(elem_hbm.at[0, 0], elem, sems.at[2 * count]))
    for copy in copies:
        copy.start()
    for copy in copies:
        copy.wait()


def stage(sink, noise, elementals):
    rows, width = sink.shape[2:]
    nev = elementals.shape[3]
    spins = width // nev
    return kernel_call(
        stage_kernel,
        1_000_000,
        in_space(HBM, 3),
        [VMEM((spins, rows, 2 * nev), BF16)] * 2 + [VMEM((2, nev, nev), BF16)],
        [DMA((4 * spins + 1,))],
    )(fixed(sink, HBM), fixed(noise, HBM), fixed(elementals, HBM))


def paired_kernel(own_ref, across_ref, out_ref):
    out_ref[0] = own_ref[...]
    out_ref[1] = across_ref[...]


def paired(own, across):
    return kernel_call(
        paired_kernel, 1_000_000, in_space(VMEM, 2), VMEM((2, *own.shape), BF16)
    )(own, across)


def fill_weights(elem, weights):
    nev = elem.shape[1]
    re, im = elem[0], elem[1]
    weights[:nev, :nev], weights[:nev, nev:] = re, -im
    weights[nev:, :nev], weights[nev:, nev:] = im, re


def apply_elemental(phi, weights, right, at):
    nev = phi.shape[1] // 2
    applied = transpose_product(weights, phi).astype(BF16)
    right[0, at : at + 2 * nev] = applied
    right[1, at : at + nev] = applied[nev:]
    right[1, at + nev : at + 2 * nev] = -applied[:nev]


def plain_product(left, right):
    return jnp.dot(left, right, preferred_element_type=F32)


def choose(wanted, held_elems, chosen):
    columns, mom = len(held_elems), lax.axis_index("mom")
    distance = lax.rem(mom // 2 - wanted // 2 + columns, columns)
    for index, elem in enumerate(held_elems):
        for across in range(2):
            @pl.when((distance == index) & (lax.rem(wanted + mom, 2) == across))
            def _():
                chosen[...] = elem[across]


def apply_all(phi, chosen, weights, right):
    fill_weights(chosen, weights)
    for spin in range(phi.shape[0]):
        apply_elemental(phi[spin], weights[...], right, spin * phi.shape[2])


def noise_rows(rho, first, rows):
    lines = slice(first, first + rows)
    return jnp.concatenate([rho[spin, lines] for spin in range(rho.shape[0])], axis=1)


def upper_sink_kernel(columns, pairs_ref, phi, rho, *refs):
    held_elems = refs[:columns]
    upper, right, chosen, weights = refs[columns:]
    choose(pairs_ref[0, 0], held_elems, chosen)
    apply_all(phi, chosen, weights, right)
    left = noise_rows(rho, 0, upper.shape[1])
    for part in range(2):
        upper[part] = plain_product(left, right[part]).astype(BF16)


def upper_sink(pairs, phi, rho, elementals, upper_rows):
    spins, rows, nev = phi.shape[0], phi.shape[1], phi.shape[2] // 2
    return kernel_call(
        functools.partial(upper_sink_kernel, len(elementals)),
        800_000_000,
        in_space(SMEM) + in_space(VMEM, 2 + len(elementals)),
        [
            VMEM((2, upper_rows, rows), BF16),
            VMEM((2, spins * 2 * nev, rows), BF16),
            VMEM((2, nev, nev), BF16),
        ],
        [VMEM((2 * nev, 2 * nev), BF16)],
    )(fixed(pairs, HBM), phi, rho, *elementals)


def lower_sink_kernel(rho, right, upper, lower, full):
    first, rows = upper.shape[1], lower.shape[1]
    left = noise_rows(rho, first, rows)
    for part in range(2):
        term = plain_product(left, right[part]).astype(BF16)
        lower[part] = term
        full[part, first:] = term
        full[part, :first] = upper[part]


def lower_sink(rho, right, upper):
    rows = rho.shape[1]
    return kernel_call(
        lower_sink_kernel,
        540_000_000,
        in_space(VMEM, 3),
        [VMEM((2, rows - upper.shape[1], rows), BF16), VMEM((2, rows, rows), BF16)],
    )(rho, right, upper)


def source_kernel(columns, pairs_ref, phi, rho, *refs):
    held_elems = refs[:columns]
    out_ref, chosen, weights, right = refs[columns:]
    choose(pairs_ref[0, 1], held_elems, chosen)
    apply_all(phi, chosen, weights, right)
    left = noise_rows(rho, 0, out_ref.shape[1])
    for part in range(2):
        out_ref[part] = plain_product(left, right[part]).astype(BF16)


def source(pairs, phi, rho, elementals):
    spins, rows, nev = phi.shape[0], phi.shape[1], phi.shape[2] // 2
    return kernel_call(
        functools.partial(source_kernel, len(elementals)),
        1_340_000_000,
        in_space(SMEM) + in_space(VMEM, 2 + len(elementals)),
        VMEM((2, rows, rows), BF16),
        [
            VMEM((2, nev, nev), BF16),
            VMEM((2 * nev, 2 * nev), BF16),
            VMEM((2, spins * 2 * nev, rows), BF16),
        ],
    )(fixed(pairs, HBM), phi, rho, *elementals)


def applied_kernel(*refs):
    *pieces, elem_ref, right, weights = refs
    nev = elem_ref.shape[1]
    fill_weights(elem_ref, weights)
    for index, piece in enumerate(pieces):
        phi = jnp.concatenate([piece[0], piece[1]], axis=1)
        apply_elemental(phi, weights[...], right, index * 2 * nev)


def applied(pieces, elemental):
    rows, nev = pieces[0].shape[1:]
    operands = [*pieces, elemental]
    return kernel_call(
        applied_kernel,
        270_000_000,
        in_space(VMEM, len(operands)),
        VMEM((2, 2 * nev * len(pieces), rows), BF16),
        [VMEM((2 * nev, 2 * nev), BF16)],
    )(*operands)


def noise_kernel(*refs):
    *pieces, right, out_ref = refs
    left = jnp.concatenate([piece[part] for piece in pieces for part in range(2)], axis=1)
    for part in range(2):
        out_ref[part] = plain_product(left, right[part]).astype(BF16)


def noise_product(pieces, right):
    rows = pieces[0].shape[1]
    return kernel_call(
        noise_kernel, 1_080_000_000, in_space(VMEM, len(pieces) + 1), VMEM((2, rows, rows), BF16)
    )(*pieces, right)


def product_kernel(jobs, *refs):
    right = refs[sum(choices for _, _, choices in jobs)]
    out_hbm, held, sems = refs[-3:]
    core = lax.rem(lax.axis_index("tm"), 2)
    copies = []
    taken = 0
    for job, (place, first, choices) in enumerate(jobs):
        lefts = refs[taken : taken + choices]
        taken += choices
        rows = lefts[0].shape[1]
        size = rows // 2 if job + 1 == len(jobs) else rows
        for start in range(0, rows, size):
            lines = pl.ds(start, size)
            left = [ref[:, lines] for ref in lefts]
            left = left[0] if choices == 1 else jnp.where(core == 0, *left)
            for part in range(2):
                if part == 0:
                    term = plain_product(left[0], right[0]) - plain_product(left[1], right[1])
                else:
                    term = plain_product(left[0], right[1]) + plain_product(left[1], right[0])
                held[job, part, lines] = term.astype(BF16)
                copies.append(
                    pltpu.make_async_copy(
                        held.at[job, part, lines],
                        out_hbm.at[0, place(core), 0, part, pl.ds(first + start, size)],
                        sems.at[len(copies)],
                    )
                )
                copies[-1].start()
    for copy in copies:
        copy.wait()


def product(jobs, right, blocks):
    rows = right.shape[1]
    lefts = [left for _, _, lefts in jobs for left in lefts]
    operands = [*lefts, right] + ([] if blocks is None else [blocks])
    return kernel_call(
        functools.partial(
            product_kernel, tuple((place, first, len(lefts)) for place, first, lefts in jobs)
        ),
        sum(2_100_000 * jobs[i][2][0].shape[1] for i in range(len(jobs))),
        in_space(VMEM, len(lefts) + 1) + ([] if blocks is None else in_space(pl.ANY)),
        HBM((1, NSEP, 1, 2, rows, rows), BF16),
        [VMEM((len(jobs), 2, rows, rows), BF16), DMA((4 * len(jobs),))],
        input_output_aliases={} if blocks is None else {len(operands) - 1: 0},
    )(*operands)


def local(sink, noise, elementals, pairs):
    times, moms = lax.axis_size("tm"), lax.axis_size("mom")
    nev = elementals.shape[3]
    columns = moms // 2

    def earlier(block, distance):
        return lax.ppermute(block, "tm", [(t, (t - distance) % times) for t in range(times)])

    def partner(block):
        return lax.ppermute(block, "tm", [(t, t ^ 1) for t in range(times)])

    def along_x(block, distance):
        route = [(m, (m // 2 + distance) % columns * 2 + m % 2) for m in range(moms)]
        return lax.ppermute(block, "mom", route)

    own = elementals[0, 0]
    across = lax.ppermute(own, "mom", [(m, m ^ 1) for m in range(moms)])
    phi, rho = outgoing(sink, noise, nev)
    phi = earlier(phi, 4)
    rho = earlier(rho, 4)
    own_phi, own_rho, own = stage(sink, noise, elementals)
    elems = [paired(own, across)]
    for distance in (1, 2, 3):
        elems.append(along_x(elems[0], distance))
    phis, rhos = [phi], [rho]
    for distance in (1, 3, 2):
        phis.append(along_x(phi, distance))
    for distance in (1, 3, 2):
        rhos.append(along_x(rho, distance))

    upper_rows = own_phi.shape[1] * 5 // 8
    upper, sink_right, sink_elemental = upper_sink(pairs, own_phi, own_rho, elems, upper_rows)
    later_elemental = earlier(sink_elemental, 4)
    two_a = earlier(upper, 2)
    lower, sink_meson = lower_sink(own_rho, sink_right, upper)
    two_b = earlier(lower, 2)
    beside = partner(sink_meson)
    source_meson = source(pairs, own_phi, own_rho, elems)

    beside_a = partner(two_a)
    right = applied(phis, later_elemental)
    four_later = noise_product(rhos, right)
    beside_four = partner(four_later)
    beside_b = partner(two_b)

    two, one_or_three, four, three_or_one = (
        lambda c: 1, lambda c: 2 * c, lambda c: 3, lambda c: 2 - 2 * c,
    )
    blocks = product([(two, 0, [two_a])], source_meson, None)
    jobs = [(four, 0, [four_later]), (three_or_one, 0, [beside_a])]
    blocks = product(jobs, source_meson, blocks)
    jobs = [(one_or_three, 0, [beside, beside_four]), (two, upper_rows, [two_b])]
    blocks = product(jobs, source_meson, blocks)
    return product([(three_or_one, upper_rows, [beside_b])], source_meson, blocks)


def solution(mesh):
    return jax.shard_map(
        local,
        mesh=mesh,
        in_specs=(
            P("tm", None, None, None),
            P("tm", None, None, None),
            P("mom", "tm", None, None, None),
            P("mom", None),
        ),
        out_specs=P("tm", None, "mom", None, None, None),
        check_vma=False,
    )
```

```python
import functools

import jax
import jax.numpy as jnp
from jax import lax
from jax.experimental import pallas as pl
from jax.experimental.pallas import tpu as pltpu
from jax.sharding import PartitionSpec as P


NSEP = 4
VMEM_LIMIT = 24 * 1024 * 1024
F32 = jnp.float32
BF16 = jnp.bfloat16
VMEM, SMEM, HBM = pltpu.VMEM, pltpu.SMEM, pltpu.HBM
DMA = pltpu.SemaphoreType.DMA


def transpose_product(left_mat, right_mat):
    return lax.dot_general(
        left_mat, right_mat, (((1,), (1,)), ((), ())), preferred_element_type=F32
    )


def in_space(space, count=1):
    return [pl.BlockSpec(memory_space=space)] * count


def fixed(array, space):
    return pltpu.with_memory_space_constraint(array, space)


def kernel_call(body, flops, in_specs, out_shape, scratch=(), **options):
    many = isinstance(out_shape, list)
    spaces = [in_space(shape.memory_space)[0] for shape in (out_shape if many else [out_shape])]
    return pl.pallas_call(
        body,
        in_specs=in_specs,
        out_specs=spaces if many else spaces[0],
        out_shape=out_shape,
        scratch_shapes=scratch,
        compiler_params=pltpu.CompilerParams(vmem_limit_bytes=VMEM_LIMIT),
        cost_estimate=pl.CostEstimate(flops=flops, bytes_accessed=3_000_000, transcendentals=0),
        **options,
    )


def outgoing_kernel(phi_hbm, rho_hbm, elem_hbm, phi_out, rho_out, elem_out, sems):
    nev = phi_out.shape[2]
    cols = pl.ds(pl.multiple_of(lax.axis_index("mom") // 2 * nev, nev), nev)
    copies = []
    for source, held in ((phi_hbm, phi_out), (rho_hbm, rho_out)):
        for part in range(2):
            copies.append(
                pltpu.make_async_copy(source.at[0, part, :, cols], held.at[part], sems.at[len(copies)])
            )
            copies[-1].start()
    copies.append(pltpu.make_async_copy(elem_hbm.at[0, 0], elem_out, sems.at[len(copies)]))
    copies[-1].start()
    for copy in copies:
        copy.wait()


def outgoing(sink, noise, elementals):
    rows, nev = sink.shape[2], elementals.shape[3]
    return kernel_call(
        outgoing_kernel,
        1_000_000,
        in_space(HBM, 3),
        [VMEM((2, rows, nev), BF16)] * 2 + [VMEM((2, nev, nev), BF16)],
        [DMA((5,))],
    )(fixed(sink, HBM), fixed(noise, HBM), fixed(elementals, HBM))


def by_spin(source, held, sems):
    spins, nev = held.shape[0], held.shape[2] // 2
    return [
        pltpu.make_async_copy(
            source.at[0, part, :, pl.ds(spin * nev, nev)],
            held.at[spin, :, pl.ds(part * nev, nev)],
            sems.at[2 * spin + part],
        )
        for spin in range(spins)
        for part in range(2)
    ]


def stage_kernel(phi_hbm, rho_hbm, phi, rho, sems):
    count = sems.shape[0] // 2
    copies = by_spin(phi_hbm, phi, sems) + by_spin(rho_hbm, rho, sems.at[pl.ds(count, count)])
    for copy in copies:
        copy.start()
    for copy in copies:
        copy.wait()


def stage(sink, noise, nev):
    rows, width = sink.shape[2:]
    spins = width // nev
    return kernel_call(
        stage_kernel,
        1_000_000,
        in_space(HBM, 2),
        [VMEM((spins, rows, 2 * nev), BF16)] * 2,
        [DMA((4 * spins,))],
    )(fixed(sink, HBM), fixed(noise, HBM))


def paired_kernel(own_ref, across_ref, out_ref):
    out_ref[0] = own_ref[...]
    out_ref[1] = across_ref[...]


def paired(own, across):
    return kernel_call(
        paired_kernel, 1_000_000, in_space(VMEM, 2), VMEM((2, *own.shape), BF16)
    )(own, across)


def fill_weights(elem, weights):
    nev = elem.shape[1]
    re, im = elem[0], elem[1]
    weights[:nev, :nev], weights[:nev, nev:] = re, -im
    weights[nev:, :nev], weights[nev:, nev:] = im, re


def apply_elemental(phi, weights, right, at):
    nev = phi.shape[1] // 2
    applied = transpose_product(weights, phi).astype(BF16)
    right[0, at : at + 2 * nev] = applied
    right[1, at : at + nev] = applied[nev:]
    right[1, at + nev : at + 2 * nev] = -applied[:nev]


def plain_product(left, right):
    return jnp.dot(left, right, preferred_element_type=F32)


def choose(wanted, held_elems, chosen):
    columns, mom = len(held_elems), lax.axis_index("mom")
    distance = lax.rem(mom // 2 - wanted // 2 + columns, columns)
    for index, elem in enumerate(held_elems):
        for across in range(2):
            @pl.when((distance == index) & (lax.rem(wanted + mom, 2) == across))
            def _():
                chosen[...] = elem[across]


def apply_all(phi, chosen, weights, right):
    fill_weights(chosen, weights)
    for spin in range(phi.shape[0]):
        apply_elemental(phi[spin], weights[...], right, spin * phi.shape[2])


def noise_rows(rho, first, rows):
    lines = slice(first, first + rows)
    return jnp.concatenate([rho[spin, lines] for spin in range(rho.shape[0])], axis=1)


def upper_sink_kernel(columns, pairs_ref, phi, rho, *refs):
    held_elems = refs[:columns]
    upper, right, chosen, weights = refs[columns:]
    choose(pairs_ref[0, 0], held_elems, chosen)
    apply_all(phi, chosen, weights, right)
    left = noise_rows(rho, 0, upper.shape[1])
    for part in range(2):
        upper[part] = plain_product(left, right[part]).astype(BF16)


def upper_sink(pairs, phi, rho, elementals, upper_rows):
    spins, rows, nev = phi.shape[0], phi.shape[1], phi.shape[2] // 2
    return kernel_call(
        functools.partial(upper_sink_kernel, len(elementals)),
        800_000_000,
        in_space(SMEM) + in_space(VMEM, 2 + len(elementals)),
        [
            VMEM((2, upper_rows, rows), BF16),
            VMEM((2, spins * 2 * nev, rows), BF16),
            VMEM((2, nev, nev), BF16),
        ],
        [VMEM((2 * nev, 2 * nev), BF16)],
    )(fixed(pairs, HBM), phi, rho, *elementals)


def lower_sink_kernel(rho, right, upper, lower, full):
    first, rows = upper.shape[1], lower.shape[1]
    left = noise_rows(rho, first, rows)
    for part in range(2):
        term = plain_product(left, right[part]).astype(BF16)
        lower[part] = term
        full[part, first:] = term
        full[part, :first] = upper[part]


def lower_sink(rho, right, upper):
    rows = rho.shape[1]
    return kernel_call(
        lower_sink_kernel,
        540_000_000,
        in_space(VMEM, 3),
        [VMEM((2, rows - upper.shape[1], rows), BF16), VMEM((2, rows, rows), BF16)],
    )(rho, right, upper)


def source_kernel(columns, pairs_ref, phi, rho, *refs):
    held_elems = refs[:columns]
    out_ref, chosen, weights, right = refs[columns:]
    choose(pairs_ref[0, 1], held_elems, chosen)
    apply_all(phi, chosen, weights, right)
    left = noise_rows(rho, 0, out_ref.shape[1])
    for part in range(2):
        out_ref[part] = plain_product(left, right[part]).astype(BF16)


def source(pairs, phi, rho, elementals):
    spins, rows, nev = phi.shape[0], phi.shape[1], phi.shape[2] // 2
    return kernel_call(
        functools.partial(source_kernel, len(elementals)),
        1_340_000_000,
        in_space(SMEM) + in_space(VMEM, 2 + len(elementals)),
        VMEM((2, rows, rows), BF16),
        [
            VMEM((2, nev, nev), BF16),
            VMEM((2 * nev, 2 * nev), BF16),
            VMEM((2, spins * 2 * nev, rows), BF16),
        ],
    )(fixed(pairs, HBM), phi, rho, *elementals)


def applied_kernel(*refs):
    *pieces, elem_ref, right, weights = refs
    nev = elem_ref.shape[1]
    fill_weights(elem_ref, weights)
    for index, piece in enumerate(pieces):
        phi = jnp.concatenate([piece[0], piece[1]], axis=1)
        apply_elemental(phi, weights[...], right, index * 2 * nev)


def applied(pieces, elemental):
    rows, nev = pieces[0].shape[1:]
    operands = [*pieces, elemental]
    return kernel_call(
        applied_kernel,
        270_000_000,
        in_space(VMEM, len(operands)),
        VMEM((2, 2 * nev * len(pieces), rows), BF16),
        [VMEM((2 * nev, 2 * nev), BF16)],
    )(*operands)


def noise_kernel(*refs):
    *pieces, right, out_ref = refs
    left = jnp.concatenate([piece[part] for piece in pieces for part in range(2)], axis=1)
    for part in range(2):
        out_ref[part] = plain_product(left, right[part]).astype(BF16)


def noise_product(pieces, right):
    rows = pieces[0].shape[1]
    return kernel_call(
        noise_kernel, 1_080_000_000, in_space(VMEM, len(pieces) + 1), VMEM((2, rows, rows), BF16)
    )(*pieces, right)


def product_kernel(jobs, pending, aliased, last_call, *refs):
    count = sum(choices for _, _, choices in jobs)
    right, waiting = refs[count], refs[count + 1]
    outs = refs[count + 1 + (pending is not None) + aliased :]
    out_hbm, kept, scratch, sems = outs[0], outs[1], outs[-2], outs[-1]
    core = lax.rem(lax.axis_index("tm"), 2)
    copies = []

    def send(source, part, place, first):
        lines = pl.ds(first, source.shape[1])
        copies.append(
            pltpu.make_async_copy(
                source.at[part], out_hbm.at[0, place(core), 0, part, lines], sems.at[len(copies)]
            )
        )
        copies[-1].start()

    if pending is not None:
        for part in range(2):
            send(waiting, part, *pending)
    taken = 0
    for job, (place, first, choices) in enumerate(jobs):
        lefts = refs[taken : taken + choices]
        taken += choices
        rows = lefts[0].shape[1]
        keep = job + 1 == len(jobs) and not last_call
        held = kept if keep else scratch.at[job, :, pl.ds(0, rows)]
        left = [ref[...] for ref in lefts]
        left = left[0] if choices == 1 else jnp.where(core == 0, *left)
        for part in range(2):
            if part == 0:
                term = plain_product(left[0], right[0]) - plain_product(left[1], right[1])
            else:
                term = plain_product(left[0], right[1]) + plain_product(left[1], right[0])
            held[part] = term.astype(BF16)
            if not keep:
                send(held, part, place, first)
    for copy in copies:
        copy.wait()


def product(jobs, right, pending, blocks, last_call=False):
    rows = right.shape[1]
    lefts = [left for _, _, lefts in jobs for left in lefts]
    operands = [*lefts, right] + ([] if pending is None else [pending[2]])
    operands += [] if blocks is None else [blocks]
    place, first, last_lefts = jobs[-1]
    outs = [HBM((1, NSEP, 1, 2, rows, rows), BF16)]
    outs += [] if last_call else [VMEM((2, last_lefts[0].shape[1], rows), BF16)]
    results = kernel_call(
        functools.partial(
            product_kernel,
            tuple((place, first, len(lefts)) for place, first, lefts in jobs),
            None if pending is None else pending[:2],
            blocks is not None,
            last_call,
        ),
        sum(2_100_000 * lefts[0].shape[1] for _, _, lefts in jobs),
        in_space(VMEM, len(lefts) + 1 + (pending is not None))
        + ([] if blocks is None else in_space(pl.ANY)),
        outs,
        [VMEM((len(jobs), 2, rows, rows), BF16), DMA((2 * len(jobs) + 2,))],
        input_output_aliases={} if blocks is None else {len(operands) - 1: 0},
    )(*operands)
    return (results[0], None) if last_call else (results[0], (place, first, results[1]))


def first_product(left, right):
    def kernel(left_ref, right_ref, out_ref):
        re, im = left_ref[0], left_ref[1]
        out_ref[0] = (plain_product(re, right_ref[0]) - plain_product(im, right_ref[1])).astype(BF16)
        out_ref[1] = (plain_product(re, right_ref[1]) + plain_product(im, right_ref[0])).astype(BF16)

    return kernel_call(kernel, 660_000_000, in_space(VMEM, 2), VMEM(left.shape, BF16))(left, right)


def local(sink, noise, elementals, pairs):
    times, moms = lax.axis_size("tm"), lax.axis_size("mom")
    nev, columns = elementals.shape[3], moms // 2

    def earlier(block, distance):
        return lax.ppermute(block, "tm", [(t, (t - distance) % times) for t in range(times)])

    def partner(block):
        return lax.ppermute(block, "tm", [(t, t ^ 1) for t in range(times)])

    def along_x(block, distance):
        route = [(m, (m // 2 + distance) % columns * 2 + m % 2) for m in range(moms)]
        return lax.ppermute(block, "mom", route)

    across = lax.ppermute(elementals[0, 0], "mom", [(m, m ^ 1) for m in range(moms)])
    phi, rho, own = outgoing(sink, noise, elementals)
    phi = earlier(phi, 4)
    rho = earlier(rho, 4)
    elems = [paired(own, across)]
    for distance in (1, 2, 3):
        elems.append(along_x(elems[0], distance))
    own_phi, own_rho = stage(sink, noise, nev)
    phis, rhos = [phi], [rho]
    for distance in (1, 3, 2):
        phis.append(along_x(phi, distance))
    for distance in (1, 3, 2):
        rhos.append(along_x(rho, distance))

    upper_rows = own_phi.shape[1] * 5 // 8
    upper, sink_right, sink_elemental = upper_sink(pairs, own_phi, own_rho, elems, upper_rows)
    later_elemental = earlier(sink_elemental, 4)
    two_a = earlier(upper, 2)
    lower, sink_meson = lower_sink(own_rho, sink_right, upper)
    two_b = earlier(lower, 2)
    beside = partner(sink_meson)
    source_meson = source(pairs, own_phi, own_rho, elems)

    beside_a = partner(two_a)
    right = applied(phis, later_elemental)
    four_later = noise_product(rhos, right)
    beside_four = partner(four_later)
    beside_b = partner(two_b)

    two, one_or_three, four, three_or_one = (
        lambda c: 1, lambda c: 2 * c, lambda c: 3, lambda c: 2 - 2 * c,
    )
    pending = (two, 0, first_product(two_a, source_meson))
    jobs = [(three_or_one, 0, [beside_a]), (four, 0, [four_later])]
    blocks, pending = product(jobs, source_meson, pending, None)
    jobs = [(two, upper_rows, [two_b]), (one_or_three, 0, [beside, beside_four])]
    blocks, pending = product(jobs, source_meson, pending, blocks)
    jobs = [(three_or_one, upper_rows, [beside_b])]
    return product(jobs, source_meson, pending, blocks, last_call=True)[0]


def solution(mesh):
    return jax.shard_map(
        local,
        mesh=mesh,
        in_specs=(
            P("tm", None, None, None),
            P("tm", None, None, None),
            P("mom", "tm", None, None, None),
            P("mom", None),
        ),
        out_specs=P("tm", None, "mom", None, None, None),
        check_vma=False,
    )
```
